256 devices in a mesh: tracts: 2 (over y), sky: 32 (over z, core), depth: 4 (over x).
Axes of the slice: x: 4, y: 2, z: 16, core: 2. Of those that a mesh axis runs over, the one named last changes fastest.
The devices are a block of a 4x16x16 slice.
Arguments:
- visit_tiles: bfloat16 [1024, 32, 64, 512], P(('tracts', 'sky', 'depth')), parts along dimension 0, may hold values from -6 to 6
- warp_matrix: bfloat16 [1024, 512, 512], P(('tracts', 'sky', 'depth')), parts along dimension 0, may hold values from -0.25 to 0.25
- flux_scale: float32 [1024], P(('tracts', 'sky', 'depth')), parts along dimension 0, may hold values from 0.3 to 3
- patch_lists: int32 [1024, 32], P(('tracts', 'sky', 'depth')), parts along dimension 0, may hold values from 0 to 127, all different within a row; in each aligned block of 4 rows (0 to 3, 4 to 7, ...) at most 2 rows name the same one
- clip_bits: int32 [1024, 32, 4, 512], P(('tracts', 'sky', 'depth')), parts along dimension 0, may hold values from -2147483648 to 2147483647, as said below
Outputs:
- coadd_mean: float32 [2, 256, 64, 512], P(None, ('tracts', 'sky'), 'depth'), parts along dimension 1
- coadd_var: float32 [2, 256, 64, 512], P(None, ('tracts', 'sky'), 'depth'), parts along dimension 1
The draws below stay inside these ranges and needn't reach their ends.
There are 2 independent parts, one for each index of `tracts`. The reference program is written for one: setup_inputs(seed, part) draws one part's arguments, and reference() takes and returns one part's arrays. A program takes and returns all parts, laid end to end along the dimension named above; each array names one. Nothing has to cross between parts.
Inputs may be any that keep to these rules, and one draw needn't show every extreme that they name: `patch_lists`: row v names the 32 different patches of visit v's blocks. In the rows of one device no patch is named more than 2 times, a bound that some block reaches there; every patch is named by some row. Bit 16 t + j of clip_bits[v, k, g, c] is 1 when clip pass t (t = 0 or 1) keeps the sample of visit v's block k at row 16 g + j, column c.
All inputs are finite; a program needn't handle non-finite values.
Results may differ from the reference program's by a relative error of at most 0.0029.
Values may be sent and summed in bfloat16 or wider, within the bound.
No kernel may reach another device: no remote copies, remote signals or barrier semaphores. Data moves between devices by JAX's collectives and lax.ppermute only.
A program may use at most 128 MiB of HBM per device.

```python
import math
import jax
import jax.numpy as jnp
import numpy as np
from jax import lax

COLUMNS = 512
ROWS = 64
VISITS_DEV = 4
CAPACITY = 2
PATCHES = 128
INTERSECTIONS = 32
VISITS = 512


def draw_clip_bits(key, part):
    word_shape = (VISITS, INTERSECTIONS, ROWS // 16, COLUMNS)

    def add_bit(position, packed):
        level = jax.random.randint(jax.random.fold_in(key, position + 7), word_shape, 0, 20, dtype=jnp.int32)
        limit = jnp.where(position < 16, 18, 17)
        kept = (level < limit).astype(jnp.int32)
        return jnp.bitwise_or(packed, jnp.left_shift(kept, position))
    return lax.fori_loop(0, 32, add_bit, jnp.zeros(word_shape, jnp.int32))


def levels(own_key, dims, shards, low, top_value):
    loudness = 1.0
    for dim, parts in shards:
        heights = jax.random.uniform(jax.random.fold_in(jax.random.fold_in(own_key, 6), dim), (parts,), jnp.float32, low / len(shards), top_value / len(shards))
        loudness = loudness * jnp.repeat(jnp.exp(heights), dims[dim] // parts).reshape((-1,) + (1,) * (len(dims) - 1 - dim))
    return loudness


def routed_block(rng, own, number, rows, amount, top, most, lean):
    sequence = jax.random.permutation(rng, amount)
    crowded, common = load_shares(amount, rows * top, most, lean, True), load_shares(amount, rows * top, most, lean, False)
    places = jnp.arange(amount)

    def named(tallies, turn):
        used = int((tallies > 0).sum())
        fixed = max(1, used // 4)
        passed = fixed + (places - fixed + turn * (used - fixed)) % max(1, amount - fixed)
        return jnp.zeros((amount,), jnp.int32).at[sequence[jnp.where(places < fixed, places, passed)]].set(jnp.asarray(tallies, jnp.int32))

    tallies = jnp.where(number % 4 == 0, named(crowded, number // 4), named(common, number - number // 4 - 1))
    mixed = jax.random.permutation(jax.random.fold_in(own, 3), amount)
    giver, receiver = mixed[0:amount // 2 * 2:2], mixed[1:amount // 2 * 2:2]
    room = jnp.minimum(tallies[giver] - 1, most - tallies[receiver]) // 2
    room = jnp.where((giver == sequence[0]) | (receiver == sequence[0]) | (tallies[receiver] == 0), 0, jnp.maximum(room, 0))
    passed = jax.random.randint(jax.random.fold_in(own, 4), (amount // 2,), 0, 1 << 20) % (room + 1)
    tallies = tallies.at[giver].add(-passed).at[receiver].add(passed)
    members = jnp.searchsorted(jnp.cumsum(tallies), jnp.arange(rows * top), side="right").astype(jnp.int32)
    listing = members.reshape(top, rows).T
    listing = listing[jax.random.permutation(jax.random.fold_in(own, 1), rows)]
    turn = jax.random.randint(jax.random.fold_in(own, 2), (rows, 1), 0, top)
    return jnp.take_along_axis(listing, (jnp.arange(top)[None, :] + turn) % top, axis=1)


def load_shares(count, total, most, lean, full):
    weights = [(1 << 20) // math.isqrt(grade ** lean) + 1 for grade in range(1, count + 1)]
    largest = most if full else min(most, max(-(-total // count), total * weights[0] // sum(weights)))
    least = 1 if total - largest >= count - 1 else 0
    counts, surplus = [largest] + [least] * (count - 1), total - largest - least * (count - 1)
    while surplus > 0:
        candidates = [i for i in range(1, count) if counts[i] < largest] or [i for i in range(1, count) if counts[i] < most]
        mass, remaining = sum([weights[i] for i in candidates]), surplus
        for i in candidates:
            extra = min(most - counts[i], max(1, remaining * weights[i] // mass), surplus)
            counts[i] = counts[i] + extra
            surplus = surplus - extra
    return np.array(counts)


def scatter_about(rng, extent, deviation, reach, cuts=(), held_as=jnp.bfloat16):
    entries = jax.random.normal(rng, extent, jnp.float32) * deviation
    if len(cuts) > 0:
        entries = levels(rng, extent, cuts, -0.22, 0.18) * entries
    return jnp.clip(entries, min=-reach, max=reach).astype(held_as)


def setup_inputs(seed: int = 0, part: int = 0) -> dict:
    key_list = jax.random.split(jax.random.key(seed), 6)
    part_splits = jax.random.split(jax.random.fold_in(key_list[5], part), 6)
    visit_tiles = scatter_about(part_splits[0], (VISITS, INTERSECTIONS, ROWS, COLUMNS), 1.0, 6.0, ((0, 128),))
    warp_matrix = scatter_about(part_splits[1], (VISITS, COLUMNS, COLUMNS), COLUMNS ** -0.5, 0.25, ((0, 128),))
    flux_scale = jnp.clip(jnp.exp(math.log(3.0) - 2.3025851 * jax.random.uniform(part_splits[2], (VISITS,), jnp.float32) ** levels(part_splits[2], (VISITS,), ((0, 128),), -0.2, 0.2)), 0.3, 3.0)
    patch_lists_keys = jax.random.split(jax.random.fold_in(part_splits[3], 1), VISITS // VISITS_DEV)
    patch_lists_turns = jax.random.permutation(jax.random.fold_in(part_splits[3], 3), VISITS // VISITS_DEV)
    patch_lists = jax.vmap(lambda own, number: routed_block(jax.random.fold_in(part_splits[3], 2), own, number, VISITS_DEV, PATCHES, INTERSECTIONS, CAPACITY, 2))(patch_lists_keys, patch_lists_turns).reshape((VISITS, INTERSECTIONS))
    clip_bits = draw_clip_bits(jax.random.fold_in(jax.random.fold_in(key_list[5], part), 71), part)
    return {"visit_tiles": visit_tiles, "warp_matrix": warp_matrix, "flux_scale": flux_scale, "patch_lists": patch_lists, "clip_bits": clip_bits}


def unpack_keep(packed, offset):
    positions = jnp.arange(16, dtype=jnp.int32) + offset
    bit_flags = jnp.bitwise_and(jnp.right_shift(packed[..., None, :], positions[:, None]), 1)
    target_shape = packed.shape[:-2] + (packed.shape[-2] * 16, packed.shape[-1])
    return bit_flags.reshape(target_shape).astype(jnp.float32)


def finish(count_first, sum_first, square_first, count_both, shift_sum, shift_square):
    first_mean = sum_first / jnp.maximum(count_first, 1.0)
    first_var = (square_first - sum_first * first_mean) / jnp.maximum(count_first - 1.0, 1.0)
    final_mean = first_mean + shift_sum / jnp.maximum(count_both, 1.0)
    final_var = (shift_square - shift_sum * shift_sum / jnp.maximum(count_both, 1.0)) / jnp.maximum(count_both - 1.0, 1.0)
    return jnp.stack([first_mean, final_mean]), jnp.stack([first_var, final_var])


def reference(visit_tiles, warp_matrix, flux_scale, patch_lists, clip_bits):
    def warp_one(member):
        tile_block, matrix, factor = member
        product = jnp.dot(tile_block.reshape(INTERSECTIONS * ROWS, COLUMNS), matrix, preferred_element_type=jnp.float32)
        return (product * factor).astype(jnp.bfloat16).reshape(INTERSECTIONS, ROWS, COLUMNS)

    warped = lax.map(warp_one, (visit_tiles, warp_matrix, flux_scale))
    initial = jnp.zeros((PATCHES, ROWS, COLUMNS), jnp.float32)

    def first_step(state_sums, member):
        counted, totals, squares = state_sums
        warped_rows, packed, targets = member
        samples = warped_rows.astype(jnp.float32)
        keep_mask = unpack_keep(packed, 0)
        return (counted.at[targets].add(keep_mask), totals.at[targets].add(keep_mask * samples),
                squares.at[targets].add(keep_mask * samples * samples)), None

    (count_first, sum_first, square_first), _ = lax.scan(first_step, (initial, initial, initial), (warped, clip_bits, patch_lists))
    first_mean = sum_first / jnp.maximum(count_first, 1.0)

    def second_step(state_sums, member):
        counted, totals, squares = state_sums
        warped_rows, packed, targets = member
        samples = warped_rows.astype(jnp.float32)
        keep_mask = unpack_keep(packed, 0) * unpack_keep(packed, 16)
        centred = samples - first_mean[targets]
        return (counted.at[targets].add(keep_mask), totals.at[targets].add(keep_mask * centred),
                squares.at[targets].add(keep_mask * centred * centred)), None

    (count_both, shift_sum, shift_square), _ = lax.scan(second_step, (initial, initial, initial), (warped, clip_bits, patch_lists))
    return finish(count_first, sum_first, square_first, count_both, shift_sum, shift_square)
```

```python
import functools

import jax
import jax.numpy as jnp
from jax import lax
from jax.experimental import pallas as pl
from jax.experimental.pallas import tpu as pltpu
from jax.sharding import Mesh
from jax.sharding import PartitionSpec as P

PATCH_DEV = 4
CORES = 2
WORD_ROWS = 16
LANES = 128
GROUP = 4
WORDS = 8
SUMS = 5
RADIX = 4096


def warp_kernel(depth, part, half, where_ref, scale_ref, tiles_ref, matrix_ref, *out_refs):
    here, core = where_ref[0], where_ref[1]
    factor = scale_ref[pl.program_id(0)]
    blocks = tiles_ref.shape[1]
    sides = []
    for h in range(CORES):
        side = core if h == 0 else 1 - core
        start = pl.multiple_of(side * half + part * LANES, LANES)
        sides.append(matrix_ref[0, :, pl.ds(start, LANES)])
    matrix = jnp.concatenate(sides, axis=1)
    for k in range(depth):
        row = pl.multiple_of(lax.rem(here + k, depth) * WORD_ROWS, WORD_ROWS)
        rows = tiles_ref[0, :, pl.ds(row, WORD_ROWS), :].reshape(blocks * WORD_ROWS, -1)
        product = jnp.dot(rows, matrix, preferred_element_type=jnp.float32) * factor
        product = product.astype(jnp.bfloat16)
        for h in range(CORES):
            piece = product[:, h * LANES : (h + 1) * LANES]
            out_refs[k * CORES + h][...] = piece.reshape(blocks, WORD_ROWS, LANES)


def warp_part(visit_tiles, warp_matrix, flux_scale, where, depth, part):
    visits, blocks, rows, columns = visit_tiles.shape
    piece = jax.ShapeDtypeStruct((visits * blocks, WORD_ROWS, LANES), jnp.bfloat16)
    return pl.pallas_call(
        functools.partial(warp_kernel, depth, part, columns // CORES),
        out_shape=[piece] * (depth * CORES),
        grid=(visits,),
        in_specs=[
            pl.BlockSpec(memory_space=pltpu.SMEM),
            pl.BlockSpec(memory_space=pltpu.SMEM),
            pl.BlockSpec((1, blocks, rows, columns), lambda v: (v, 0, 0, 0)),
            pl.BlockSpec((1, columns, columns), lambda v: (v, 0, 0)),
        ],
        out_specs=[pl.BlockSpec((blocks, WORD_ROWS, LANES), lambda v: (v, 0, 0))] * (depth * CORES),
        name=f"warp_part{part}",
    )(where, flux_scale, visit_tiles, warp_matrix)


def sums_kernel(part, sources, patch_ref, *refs):
    tile_refs, bit_refs, out_ref = refs[:sources], refs[sources : 2 * sources], refs[-1]
    patches = out_ref.shape[0]
    entries = tile_refs[0].shape[0]
    positions = lax.broadcasted_iota(jnp.int32, (WORD_ROWS, LANES), 0)

    def clear(p, _):
        out_ref[p] = jnp.zeros(out_ref.shape[1:], jnp.float32)
        return 0

    lax.fori_loop(0, patches, clear, 0)
    for s in range(sources):

        def step(g, _, s=s):
            base = pl.multiple_of(g * WORDS, WORDS)
            words = bit_refs[s][pl.ds(base, WORDS), pl.ds(part * LANES, LANES)]
            for j in range(0, WORDS, GROUP):
                ids = [patch_ref[s, base + j + i] for i in range(GROUP)]
                held = [out_ref[p] for p in ids]
                for i in range(GROUP):
                    samples = tile_refs[s][base + j + i].astype(jnp.float32)
                    word = jnp.broadcast_to(words[j + i : j + i + 1], (WORD_ROWS, LANES))
                    kept = lax.bitwise_and(lax.shift_right_arithmetic(word, positions), 1)
                    both = lax.bitwise_and(
                        lax.shift_right_arithmetic(word, positions + WORD_ROWS), kept
                    )
                    counts = (kept + both * RADIX).astype(jnp.float32)
                    square = samples * samples
                    one, two = kept != 0, both != 0
                    out_ref[ids[i], 0] = held[i][0] + counts
                    out_ref[ids[i], 1] = held[i][1] + jnp.where(one, samples, 0.0)
                    out_ref[ids[i], 2] = held[i][2] + jnp.where(one, square, 0.0)
                    out_ref[ids[i], 3] = held[i][3] + jnp.where(two, samples, 0.0)
                    out_ref[ids[i], 4] = held[i][4] + jnp.where(two, square, 0.0)
            return 0

        lax.fori_loop(0, entries // WORDS, step, 0)


def sums_part(tiles, bits, patch_ids, patches, part):
    sources = len(tiles)
    return pl.pallas_call(
        functools.partial(sums_kernel, part, sources),
        out_shape=jax.ShapeDtypeStruct((patches, SUMS, WORD_ROWS, LANES), jnp.float32),
        in_specs=[pl.BlockSpec(memory_space=pltpu.SMEM)]
        + [pl.BlockSpec(memory_space=pltpu.VMEM)] * (2 * sources),
        out_specs=pl.BlockSpec(memory_space=pltpu.VMEM),
        name=f"sums_part{part}",
    )(patch_ids, *tiles, *bits)


def finish(sums):
    packed, sum_first, square_first, sum_both, square_both = (sums[:, i] for i in range(SUMS))
    count_both = jnp.floor(packed * (1.0 / RADIX))
    count_first = packed - count_both * RADIX
    first_mean = sum_first / jnp.maximum(count_first, 1.0)
    first_var = (square_first - sum_first * first_mean) / jnp.maximum(count_first - 1.0, 1.0)
    some = jnp.maximum(count_both, 1.0)
    shift_sum = sum_both - count_both * first_mean
    final_mean = first_mean + shift_sum / some
    final_var = (square_both - sum_both * (sum_both / some)) / jnp.maximum(count_both - 1.0, 1.0)
    return jnp.stack([first_mean, final_mean, first_var, final_var])


def per_device(visit_tiles, warp_matrix, flux_scale, patch_lists, clip_bits):
    visits, blocks, _, columns = visit_tiles.shape
    entries = visits * blocks
    chips, depth = lax.axis_size("chip"), lax.axis_size("depth")
    patches = PATCH_DEV * CORES * chips
    half = columns // CORES
    here, core = lax.axis_index("depth"), lax.axis_index("core")
    where = jnp.stack([here, core]).astype(jnp.int32)

    def place(d, c):
        return c * depth + d

    def send(value, k, h):
        if k == 0 and h == 0:
            return value
        pairs = [
            (place(d, c), place((d + k) % depth, c ^ h)) for c in range(CORES) for d in range(depth)
        ]
        return lax.ppermute(value, ("core", "depth"), pairs)

    words = clip_bits.reshape(entries, depth, CORES, half).transpose(1, 2, 0, 3)
    names = jnp.zeros((8, half), jnp.int32).at[0, :entries].set(patch_lists.reshape(entries))
    bits = []
    for k in range(depth):
        for h in range(CORES):
            message = words[lax.rem(here + k, depth), core if h == 0 else 1 - core]
            bits.append(send(jnp.concatenate([message, names]), k, h))
    patch_ids = jnp.stack([b[entries, :entries] for b in bits])

    parts = []
    for part in range(half // LANES):
        pieces = warp_part(visit_tiles, warp_matrix, flux_scale, where, depth, part)
        tiles = [send(pieces[k * CORES + h], k, h) for k in range(depth) for h in range(CORES)]
        sums = sums_part(tiles, bits, patch_ids, patches, part)
        parts.append(lax.psum_scatter(sums, "chip", scatter_dimension=0, tiled=True))
    results = finish(jnp.concatenate(parts, axis=-1))
    results = results.reshape(4, CORES, PATCH_DEV, WORD_ROWS, half)
    own, other = results[:, core], results[:, 1 - core]
    other = lax.ppermute(other, "core", [(c, c ^ 1) for c in range(CORES)])
    low, high = jnp.where(core == 0, own, other), jnp.where(core == 0, other, own)
    joined = jnp.concatenate([low, high], axis=-1)
    return joined[:2], joined[2:]


def solution(mesh):
    tracts, sky, depth = mesh.devices.shape
    fine = Mesh(
        mesh.devices.reshape(tracts, sky // CORES, CORES, depth),
        ("tracts", "chip", "core", "depth"),
    )
    every = ("tracts", "chip", "core", "depth")
    placed = (
        P(every, None, None, None),
        P(every, None, None),
        P(every),
        P(every, None),
        P(every, None, None, None),
    )
    out = P(None, ("tracts", "chip", "core"), "depth", None)
    return jax.shard_map(
        per_device, mesh=fine, in_specs=placed, out_specs=(out, out), check_vma=False
    )
```

```python
import functools

import jax
import jax.numpy as jnp
from jax import lax
from jax.experimental import pallas as pl
from jax.experimental.pallas import tpu as pltpu
from jax.sharding import Mesh
from jax.sharding import PartitionSpec as P

PATCH_DEV = 4
CORES = 2
WORD_ROWS = 16
LANES = 128
ROWS = 8
WORDS = 8
SUMS = 5
RADIX = 4096
CHUNKS = (((0, 0),), ((1, 0), (0, 1)), ((1, 1),))
TICKS = ((5,), (3, 2), (0, 6, 8))


def warp_kernel(depth, where_ref, scale_ref, tiles_ref, matrix_ref, *out_refs):
    here, core = where_ref[0], where_ref[1]
    factor = scale_ref[pl.program_id(0)]
    blocks, columns = tiles_ref.shape[1], tiles_ref.shape[3]
    half = columns // CORES
    low = pl.multiple_of(core * half, half)
    high = pl.multiple_of((1 - core) * half, half)
    matrix = jnp.concatenate(
        [matrix_ref[0, :, pl.ds(low, half)], matrix_ref[0, :, pl.ds(high, half)]], axis=1
    )
    for k in range(depth):
        row = pl.multiple_of(lax.rem(here + k, depth) * WORD_ROWS, WORD_ROWS)
        rows = tiles_ref[0, :, pl.ds(row, WORD_ROWS), :].reshape(blocks * WORD_ROWS, columns)
        product = jnp.dot(rows, matrix, preferred_element_type=jnp.float32) * factor
        product = product.reshape(blocks, WORD_ROWS, columns)
        for n, units in enumerate(CHUNKS):
            for h in range(CORES):
                out = out_refs[(n * depth + k) * CORES + h]
                pieces = []
                for high_rows, part in units:
                    start = h * half + part * LANES
                    pieces.append(
                        product[:, high_rows * ROWS : (high_rows + 1) * ROWS, start : start + LANES]
                    )
                piece = pieces[0] if len(pieces) == 1 else jnp.concatenate(pieces, axis=1)
                out[...] = piece.astype(jnp.bfloat16)


def warp_all(visit_tiles, warp_matrix, flux_scale, where, depth):
    visits, blocks, rows, columns = visit_tiles.shape
    heights = [ROWS * len(units) for units in CHUNKS for _ in range(depth * CORES)]
    return pl.pallas_call(
        functools.partial(warp_kernel, depth),
        out_shape=[
            jax.ShapeDtypeStruct((visits * blocks, height, LANES), jnp.bfloat16)
            for height in heights
        ],
        grid=(visits,),
        in_specs=[
            pl.BlockSpec(memory_space=pltpu.SMEM),
            pl.BlockSpec(memory_space=pltpu.SMEM),
            pl.BlockSpec((1, blocks, rows, columns), lambda v: (v, 0, 0, 0)),
            pl.BlockSpec((1, columns, columns), lambda v: (v, 0, 0)),
        ],
        out_specs=[pl.BlockSpec((blocks, height, LANES), lambda v: (v, 0, 0)) for height in heights],
        cost_estimate=pl.CostEstimate(
            flops=2 * visits * blocks * rows * columns * columns,
            bytes_accessed=4 * visits * blocks * rows * columns,
            transcendentals=0,
        ),
        name="warp_all",
    )(where, flux_scale, visit_tiles, warp_matrix)


def sums_kernel(units, sources, patch_ref, *refs):
    tile_refs, bit_refs, out_ref = refs[:sources], refs[sources : 2 * sources], refs[-1]
    patches = out_ref.shape[0]
    entries = tile_refs[0].shape[0]
    group = WORDS // len(units)
    positions = lax.broadcasted_iota(jnp.int32, (ROWS, LANES), 0)

    def clear(p, _):
        out_ref[p] = jnp.zeros(out_ref.shape[1:], jnp.float32)
        return 0

    lax.fori_loop(0, patches, clear, 0)
    for s in range(sources):

        def step(g, _, s=s):
            base = pl.multiple_of(g * WORDS, WORDS)
            words = [
                bit_refs[s][pl.ds(base, WORDS), pl.ds(part * LANES, LANES)] for _, part in units
            ]
            for j in range(0, WORDS, group):
                ids = [patch_ref[s, base + j + i] for i in range(group)]
                held = [out_ref[p] for p in ids]
                for i in range(group):
                    block = tile_refs[s][base + j + i].astype(jnp.float32)
                    for n, (high_rows, _) in enumerate(units):
                        rows = slice(n * ROWS, (n + 1) * ROWS)
                        samples = block[rows]
                        word = jnp.broadcast_to(words[n][j + i : j + i + 1], (ROWS, LANES))
                        shift = positions + high_rows * ROWS
                        kept = lax.bitwise_and(lax.shift_right_arithmetic(word, shift), 1)
                        both = lax.bitwise_and(
                            lax.shift_right_arithmetic(word, shift + WORD_ROWS), kept
                        )
                        counts = (kept + both * RADIX).astype(jnp.float32)
                        square = samples * samples
                        one, two = kept != 0, both != 0
                        old = held[i][:, rows]
                        out_ref[ids[i], 0, rows] = old[0] + counts
                        out_ref[ids[i], 1, rows] = old[1] + jnp.where(one, samples, 0.0)
                        out_ref[ids[i], 2, rows] = old[2] + jnp.where(one, square, 0.0)
                        out_ref[ids[i], 3, rows] = old[3] + jnp.where(two, samples, 0.0)
                        out_ref[ids[i], 4, rows] = old[4] + jnp.where(two, square, 0.0)
            return 0

        lax.fori_loop(0, entries // WORDS, step, 0)


def sums_part(tiles, bits, patch_ids, patches, units):
    sources, entries, height = len(tiles), tiles[0].shape[0], ROWS * len(units)
    return pl.pallas_call(
        functools.partial(sums_kernel, units, sources),
        out_shape=jax.ShapeDtypeStruct((patches, SUMS, height, LANES), jnp.float32),
        in_specs=[pl.BlockSpec(memory_space=pltpu.SMEM)]
        + [pl.BlockSpec(memory_space=pltpu.VMEM)] * (2 * sources),
        out_specs=pl.BlockSpec(memory_space=pltpu.VMEM),
        cost_estimate=pl.CostEstimate(
            flops=50 * sources * entries * height * LANES,
            bytes_accessed=4 * patches * SUMS * height * LANES,
            transcendentals=0,
        ),
        name="sums_part",
    )(patch_ids, *tiles, *bits)


class Chain:

    def __init__(self, sums):
        self.chips = lax.axis_size("chip")
        self.here = lax.axis_index("chip")
        self.own = PATCH_DEV * CORES
        self.sums = sums
        self.reach = self.chips // 2
        self.step = 0
        self.came = [None, None]

    def local(self, offset):
        start = lax.rem(self.here + offset + self.chips, self.chips) * self.own
        return lax.dynamic_slice_in_dim(self.sums, start, self.own, 0)

    def advance(self):
        cut = self.own // 2
        went = []
        for side, sign in enumerate((1, -1)):
            mine = self.local(sign * (self.reach - self.step))
            came = self.came[side]
            if self.step == 0:
                mine = mine[:cut] if side == 0 else mine[cut:]
            elif self.step == 1:
                if side == 0:
                    mine = jnp.concatenate([mine[:cut] + came, mine[cut:]])
                else:
                    mine = jnp.concatenate([mine[:cut], mine[cut:] + came])
            else:
                mine = mine + came
            pairs = [(i, (i + sign) % self.chips) for i in range(self.chips)]
            went.append(lax.ppermute(mine, "chip", pairs))
        self.came = list(lax.optimization_barrier(tuple(went)))
        self.step += 1

    def total(self):
        return self.local(0) + self.came[0] + self.came[1]


def finish(sums):
    packed, sum_first, square_first, sum_both, square_both = (sums[:, i] for i in range(SUMS))
    count_both = jnp.floor(packed * (1.0 / RADIX))
    count_first = packed - count_both * RADIX
    first_mean = sum_first / jnp.maximum(count_first, 1.0)
    first_var = (square_first - sum_first * first_mean) / jnp.maximum(count_first - 1.0, 1.0)
    some = jnp.maximum(count_both, 1.0)
    shift_sum = sum_both - count_both * first_mean
    final_mean = first_mean + shift_sum / some
    final_var = (square_both - sum_both * (sum_both / some)) / jnp.maximum(count_both - 1.0, 1.0)
    return jnp.stack([first_mean, final_mean, first_var, final_var])


def per_device(visit_tiles, warp_matrix, flux_scale, patch_lists, clip_bits):
    visits, blocks, _, columns = visit_tiles.shape
    entries = visits * blocks
    chips, depth = lax.axis_size("chip"), lax.axis_size("depth")
    patches = PATCH_DEV * CORES * chips
    half = columns // CORES
    here, core = lax.axis_index("depth"), lax.axis_index("core")
    where = jnp.stack([here, core]).astype(jnp.int32)

    def place(d, c):
        return c * depth + d

    def send(value, k, h):
        if k == 0 and h == 0:
            return value
        pairs = [
            (place(d, c), place((d + k) % depth, c ^ h)) for c in range(CORES) for d in range(depth)
        ]
        return lax.ppermute(value, ("core", "depth"), pairs)

    words = clip_bits.reshape(entries, depth, CORES, half).transpose(1, 2, 0, 3)
    names = jnp.zeros((8, half), jnp.int32).at[0, :entries].set(patch_lists.reshape(entries))
    bits = []
    for k in range(depth):
        for h in range(CORES):
            message = words[lax.rem(here + k, depth), core if h == 0 else 1 - core]
            bits.append(jnp.concatenate([message, names]))
    where, bits = lax.optimization_barrier((where, bits))
    bits = [send(bits[k * CORES + h], k, h) for k in range(depth) for h in range(CORES)]
    patch_ids = jnp.stack([b[entries, :entries] for b in bits])

    pieces = warp_all(visit_tiles, warp_matrix, flux_scale, where, depth)
    sources = depth * CORES
    tiles = []
    for n in range(len(CHUNKS)):
        mine = pieces[n * sources : (n + 1) * sources]
        tiles.append([send(mine[k * CORES + h], k, h) for k in range(depth) for h in range(CORES)])
    chains = []
    for n, units in enumerate(CHUNKS):
        if n:
            waits = [chain.came for chain in chains]
            tiles[n], waits = lax.optimization_barrier((tiles[n], waits))
            for chain, came in zip(chains, waits):
                chain.came = came
        chains.append(Chain(sums_part(tiles[n], bits, patch_ids, patches, units)))
        for ticks, chain in zip(TICKS[n], chains):
            for _ in range(ticks):
                chain.advance()
    squares = {}
    for chain, units in zip(chains, CHUNKS):
        results = finish(chain.total())
        results = results.reshape(4, CORES, PATCH_DEV, ROWS * len(units), LANES)
        own, other = results[:, core], results[:, 1 - core]
        other = lax.ppermute(other, "core", [(c, c ^ 1) for c in range(CORES)])
        low, high = jnp.where(core == 0, own, other), jnp.where(core == 0, other, own)
        for n, unit in enumerate(units):
            rows = slice(n * ROWS, (n + 1) * ROWS)
            squares[unit] = (low[:, :, rows], high[:, :, rows])
    joined = jnp.concatenate(
        [
            jnp.concatenate(
                [squares[r, q][c] for c in range(CORES) for q in range(half // LANES)], axis=-1
            )
            for r in range(WORD_ROWS // ROWS)
        ],
        axis=-2,
    )
    return joined[:2], joined[2:]


def solution(mesh):
    tracts, sky, depth = mesh.devices.shape
    fine = Mesh(
        mesh.devices.reshape(tracts, sky // CORES, CORES, depth),
        ("tracts", "chip", "core", "depth"),
    )
    every = ("tracts", "chip", "core", "depth")
    placed = (
        P(every, None, None, None),
        P(every, None, None),
        P(every),
        P(every, None),
        P(every, None, None, None),
    )
    out = P(None, ("tracts", "chip", "core"), "depth", None)

    return jax.shard_map(
        per_device, mesh=fine, in_specs=placed, out_specs=(out, out), check_vma=False
    )
```

```python
import functools

import jax
import jax.numpy as jnp
from jax import lax
from jax.experimental import pallas as pl
from jax.experimental.pallas import tpu as pltpu
from jax.sharding import Mesh
from jax.sharding import PartitionSpec as P

PATCH_DEV = 4
CORES = 2
WORD_ROWS = 16
LANES = 128
ROWS = 8
WORDS = 8
SUMS = 5
RADIX = 4096
CHUNKS = (((0, 0),), ((1, 0), (0, 1)), ((1, 1),))


def warp_kernel(depth, where_ref, scale_ref, tiles_ref, matrix_ref, *out_refs):
    here, core = where_ref[0], where_ref[1]
    factor = scale_ref[pl.program_id(0)]
    blocks, columns = tiles_ref.shape[1], tiles_ref.shape[3]
    half = columns // CORES
    low = pl.multiple_of(core * half, half)
    high = pl.multiple_of((1 - core) * half, half)
    matrix = jnp.concatenate(
        [matrix_ref[0, :, pl.ds(low, half)], matrix_ref[0, :, pl.ds(high, half)]], axis=1
    )
    for k in range(depth):
        row = pl.multiple_of(lax.rem(here + k, depth) * WORD_ROWS, WORD_ROWS)
        rows = tiles_ref[0, :, pl.ds(row, WORD_ROWS), :].reshape(blocks * WORD_ROWS, columns)
        product = jnp.dot(rows, matrix, preferred_element_type=jnp.float32) * factor
        product = product.reshape(blocks, WORD_ROWS, columns)
        for n, units in enumerate(CHUNKS):
            for h in range(CORES):
                out = out_refs[(n * depth + k) * CORES + h]
                pieces = []
                for high_rows, part in units:
                    start = h * half + part * LANES
                    pieces.append(
                        product[:, high_rows * ROWS : (high_rows + 1) * ROWS, start : start + LANES]
                    )
                piece = pieces[0] if len(pieces) == 1 else jnp.concatenate(pieces, axis=1)
                out[...] = piece.astype(jnp.bfloat16)


def warp_all(visit_tiles, warp_matrix, flux_scale, where, depth):
    visits, blocks, rows, columns = visit_tiles.shape
    heights = [ROWS * len(units) for units in CHUNKS for _ in range(depth * CORES)]
    return pl.pallas_call(
        functools.partial(warp_kernel, depth),
        out_shape=[
            jax.ShapeDtypeStruct((visits * blocks, height, LANES), jnp.bfloat16)
            for height in heights
        ],
        grid=(visits,),
        in_specs=[
            pl.BlockSpec(memory_space=pltpu.SMEM),
            pl.BlockSpec(memory_space=pltpu.SMEM),
            pl.BlockSpec((1, blocks, rows, columns), lambda v: (v, 0, 0, 0)),
            pl.BlockSpec((1, columns, columns), lambda v: (v, 0, 0)),
        ],
        out_specs=[pl.BlockSpec((blocks, height, LANES), lambda v: (v, 0, 0)) for height in heights],
        cost_estimate=pl.CostEstimate(
            flops=2 * visits * blocks * rows * columns * columns,
            bytes_accessed=4 * visits * blocks * rows * columns,
            transcendentals=0,
        ),
        name="warp_all",
    )(where, flux_scale, visit_tiles, warp_matrix)


def sums_kernel(units, sources, patch_ref, *refs):
    tile_refs, bit_refs, out_ref = refs[:sources], refs[sources : 2 * sources], refs[-1]
    patches = out_ref.shape[0]
    entries = tile_refs[0].shape[0]
    group = 4
    positions = lax.broadcasted_iota(jnp.int32, (ROWS, LANES), 0)
    first_masks, second_masks = [], []
    for high_rows, _ in units:
        first_masks.append(lax.shift_left(jnp.ones_like(positions), positions + high_rows * ROWS))
        second_masks.append(lax.shift_left(first_masks[-1], jnp.full_like(positions, WORD_ROWS)))

    def clear(p, _):
        out_ref[p] = jnp.zeros(out_ref.shape[1:], jnp.float32)
        return 0

    lax.fori_loop(0, patches, clear, 0)
    for s in range(sources):

        def step(g, _, s=s):
            base = pl.multiple_of(g * WORDS, WORDS)
            words = [
                bit_refs[s][pl.ds(base, WORDS), pl.ds(part * LANES, LANES)] for _, part in units
            ]
            for j in range(0, WORDS, group):
                ids = [patch_ref[s, base + j + i] for i in range(group)]
                held = [out_ref[p] for p in ids]
                for i in range(group):
                    block = tile_refs[s][base + j + i].astype(jnp.float32)
                    for n, (high_rows, _) in enumerate(units):
                        rows = slice(n * ROWS, (n + 1) * ROWS)
                        samples = block[rows]
                        word = jnp.broadcast_to(words[n][j + i : j + i + 1], (ROWS, LANES))
                        one = lax.bitwise_and(word, first_masks[n]) != 0
                        two = one & (lax.bitwise_and(word, second_masks[n]) != 0)
                        counts = jnp.where(two, 1.0 + RADIX, jnp.where(one, 1.0, 0.0))
                        square = samples * samples
                        old = held[i][:, rows]
                        out_ref[ids[i], 0, rows] = old[0] + counts
                        out_ref[ids[i], 1, rows] = old[1] + jnp.where(one, samples, 0.0)
                        out_ref[ids[i], 2, rows] = old[2] + jnp.where(one, square, 0.0)
                        out_ref[ids[i], 3, rows] = old[3] + jnp.where(two, samples, 0.0)
                        out_ref[ids[i], 4, rows] = old[4] + jnp.where(two, square, 0.0)
            return 0

        lax.fori_loop(0, entries // WORDS, step, 0)


def sums_part(tiles, bits, patch_ids, patches, units):
    sources, entries, height = len(tiles), tiles[0].shape[0], ROWS * len(units)
    return pl.pallas_call(
        functools.partial(sums_kernel, units, sources),
        out_shape=jax.ShapeDtypeStruct((patches, SUMS, height, LANES), jnp.float32),
        in_specs=[pl.BlockSpec(memory_space=pltpu.SMEM)]
        + [pl.BlockSpec(memory_space=pltpu.VMEM)] * (2 * sources),
        out_specs=pl.BlockSpec(memory_space=pltpu.VMEM),
        cost_estimate=pl.CostEstimate(
            flops=50 * sources * entries * height * LANES,
            bytes_accessed=4 * patches * SUMS * height * LANES,
            transcendentals=0,
        ),
        name="sums_part",
    )(patch_ids, *tiles, *bits)


class Chain:

    def __init__(self, sums):
        self.chips = lax.axis_size("chip")
        self.here = lax.axis_index("chip")
        self.own = PATCH_DEV * CORES
        self.sums = sums
        self.reach = self.chips // 2
        self.step = 0
        self.came = [None, None]

    def local(self, offset):
        start = lax.rem(self.here + offset + self.chips, self.chips) * self.own
        return lax.dynamic_slice_in_dim(self.sums, start, self.own, 0)

    def advance(self):
        cut = self.own // 2
        went = []
        for side, sign in enumerate((1, -1)):
            mine = self.local(sign * (self.reach - self.step))
            came = self.came[side]
            if self.step == 0:
                mine = mine[:cut] if side == 0 else mine[cut:]
            elif self.step == 1:
                if side == 0:
                    mine = jnp.concatenate([mine[:cut] + came, mine[cut:]])
                else:
                    mine = jnp.concatenate([mine[:cut], mine[cut:] + came])
            else:
                mine = mine + came
            pairs = [(i, (i + sign) % self.chips) for i in range(self.chips)]
            went.append(lax.ppermute(mine, "chip", pairs))
        self.came = list(lax.optimization_barrier(tuple(went)))
        self.step += 1

    def total(self):
        return self.local(0) + self.came[0] + self.came[1]


def finish(sums):
    packed, sum_first, square_first, sum_both, square_both = (sums[:, i] for i in range(SUMS))
    count_both = jnp.floor(packed * (1.0 / RADIX))
    count_first = packed - count_both * RADIX
    first_mean = sum_first / jnp.maximum(count_first, 1.0)
    first_var = (square_first - sum_first * first_mean) / jnp.maximum(count_first - 1.0, 1.0)
    some = jnp.maximum(count_both, 1.0)
    shift_sum = sum_both - count_both * first_mean
    final_mean = first_mean + shift_sum / some
    final_var = (square_both - sum_both * (sum_both / some)) / jnp.maximum(count_both - 1.0, 1.0)
    return jnp.stack([first_mean, final_mean, first_var, final_var])


def per_device(visit_tiles, warp_matrix, flux_scale, patch_lists, clip_bits):
    visits, blocks, _, columns = visit_tiles.shape
    entries = visits * blocks
    chips, depth = lax.axis_size("chip"), lax.axis_size("depth")
    patches = PATCH_DEV * CORES * chips
    half = columns // CORES
    here, core = lax.axis_index("depth"), lax.axis_index("core")
    where = jnp.stack([here, core]).astype(jnp.int32)

    def place(d, c):
        return c * depth + d

    def send(value, k, h):
        if k == 0 and h == 0:
            return value
        pairs = [
            (place(d, c), place((d + k) % depth, c ^ h)) for c in range(CORES) for d in range(depth)
        ]
        return lax.ppermute(value, ("core", "depth"), pairs)

    words = clip_bits.reshape(entries, depth, columns)
    names = jnp.zeros((8, half), jnp.int32).at[0, :entries].set(patch_lists.reshape(entries))
    bits = []
    for k in range(depth):
        for h in range(CORES):
            start = (core if h == 0 else 1 - core) * half
            message = lax.dynamic_slice(
                words, (0, lax.rem(here + k, depth), start), (entries, 1, half)
            )
            bits.append(jnp.concatenate([message.reshape(entries, half), names]))
    where, bits = lax.optimization_barrier((where, bits))
    bits = [send(bits[k * CORES + h], k, h) for k in range(depth) for h in range(CORES)]
    patch_ids = jnp.stack([b[entries, :entries] for b in bits])

    pieces = warp_all(visit_tiles, warp_matrix, flux_scale, where, depth)
    sources = depth * CORES
    tiles = []
    for n in range(len(CHUNKS)):
        mine = pieces[n * sources : (n + 1) * sources]
        tiles.append([send(mine[k * CORES + h], k, h) for k in range(depth) for h in range(CORES)])
    totals = []
    for n, units in enumerate(CHUNKS):
        sums = sums_part(tiles[n], bits, patch_ids, patches, units)
        if n + 1 < len(CHUNKS):
            totals.append(lax.psum_scatter(sums, "chip", scatter_dimension=0, tiled=True))
        else:
            chain = Chain(sums)
            for _ in range(chips // 2):
                chain.advance()
            totals.append(chain.total())
    squares = {}
    for total, units in zip(totals, CHUNKS):
        results = finish(total)
        for n, unit in enumerate(units):
            squares[unit] = results[:, :, n * ROWS : (n + 1) * ROWS]
    results = jnp.concatenate(
        [
            jnp.concatenate([squares[r, q] for q in range(half // LANES)], axis=-1)
            for r in range(WORD_ROWS // ROWS)
        ],
        axis=-2,
    ).reshape(4, CORES, PATCH_DEV, WORD_ROWS, half)
    own, other = results[:, core], results[:, 1 - core]
    other = lax.ppermute(other, "core", [(c, c ^ 1) for c in range(CORES)])
    low, high = jnp.where(core == 0, own, other), jnp.where(core == 0, other, own)
    joined = jnp.concatenate([low, high], axis=-1)
    return joined[:2], joined[2:]


def solution(mesh):
    tracts, sky, depth = mesh.devices.shape
    fine = Mesh(
        mesh.devices.reshape(tracts, sky // CORES, CORES, depth),
        ("tracts", "chip", "core", "depth"),
    )
    every = ("tracts", "chip", "core", "depth")
    placed = (
        P(every, None, None, None),
        P(every, None, None),
        P(every),
        P(every, None),
        P(every, None, None, None),
    )
    out = P(None, ("tracts", "chip", "core"), "depth", None)

    return jax.shard_map(
        per_device, mesh=fine, in_specs=placed, out_specs=(out, out), check_vma=False
    )
```

```python
import functools

import jax
import jax.numpy as jnp
from jax import lax
from jax.experimental import pallas as pl
from jax.experimental.pallas import tpu as pltpu
from jax.sharding import Mesh
from jax.sharding import PartitionSpec as P

PATCH_DEV = 4
CORES = 2
WORD_ROWS = 16
LANES = 128
ROWS = 8
WORDS = 8
SUMS = 5
RADIX = 4096
CHUNKS = (((0, 0),), ((1, 0), (0, 1)), ((1, 1),))


def warp_kernel(depth, chunks, where_ref, scale_ref, tiles_ref, matrix_ref, *out_refs):
    here, core = where_ref[0], where_ref[1]
    factor = scale_ref[pl.program_id(0)]
    blocks, columns = tiles_ref.shape[1], tiles_ref.shape[3]
    half = columns // CORES
    width = LANES * (1 + max(part for units in chunks for _, part in units))
    low = pl.multiple_of(core * half, half)
    high = pl.multiple_of((1 - core) * half, half)
    matrix = jnp.concatenate(
        [matrix_ref[0, :, pl.ds(low, width)], matrix_ref[0, :, pl.ds(high, width)]], axis=1
    )
    for k in range(depth):
        row = pl.multiple_of(lax.rem(here + k, depth) * WORD_ROWS, WORD_ROWS)
        rows = tiles_ref[0, :, pl.ds(row, WORD_ROWS), :].reshape(blocks * WORD_ROWS, columns)
        product = jnp.dot(rows, matrix, preferred_element_type=jnp.float32) * factor
        product = product.reshape(blocks, WORD_ROWS, CORES * width)
        for n, units in enumerate(chunks):
            for h in range(CORES):
                out = out_refs[(n * depth + k) * CORES + h]
                pieces = []
                for high_rows, part in units:
                    start = h * width + part * LANES
                    pieces.append(
                        product[:, high_rows * ROWS : (high_rows + 1) * ROWS, start : start + LANES]
                    )
                piece = pieces[0] if len(pieces) == 1 else jnp.concatenate(pieces, axis=1)
                out[...] = piece.astype(jnp.bfloat16)


def warp_some(visit_tiles, warp_matrix, flux_scale, where, depth, chunks):
    visits, blocks, rows, columns = visit_tiles.shape
    heights = [ROWS * len(units) for units in chunks for _ in range(depth * CORES)]
    return pl.pallas_call(
        functools.partial(warp_kernel, depth, chunks),
        out_shape=[
            jax.ShapeDtypeStruct((visits * blocks, height, LANES), jnp.bfloat16)
            for height in heights
        ],
        grid=(visits,),
        in_specs=[
            pl.BlockSpec(memory_space=pltpu.SMEM),
            pl.BlockSpec(memory_space=pltpu.SMEM),
            pl.BlockSpec((1, blocks, rows, columns), lambda v: (v, 0, 0, 0)),
            pl.BlockSpec((1, columns, columns), lambda v: (v, 0, 0)),
        ],
        out_specs=[pl.BlockSpec((blocks, height, LANES), lambda v: (v, 0, 0)) for height in heights],
        cost_estimate=pl.CostEstimate(
            flops=2 * visits * blocks * rows * columns * columns,
            bytes_accessed=4 * visits * blocks * rows * columns,
            transcendentals=0,
        ),
        name="warp_some",
    )(where, flux_scale, visit_tiles, warp_matrix)


def sums_kernel(units, sources, patch_ref, *refs):
    tile_refs, bit_refs, out_ref = refs[:sources], refs[sources : 2 * sources], refs[-1]
    patches = out_ref.shape[0]
    entries = tile_refs[0].shape[0]
    group = 4
    positions = lax.broadcasted_iota(jnp.int32, (ROWS, LANES), 0)
    first_masks, second_masks = [], []
    for high_rows, _ in units:
        first_masks.append(lax.shift_left(jnp.ones_like(positions), positions + high_rows * ROWS))
        second_masks.append(lax.shift_left(first_masks[-1], jnp.full_like(positions, WORD_ROWS)))

    def clear(p, _):
        out_ref[p] = jnp.zeros(out_ref.shape[1:], jnp.float32)
        return 0

    lax.fori_loop(0, patches, clear, 0)
    for s in range(sources):

        def step(g, _, s=s):
            base = pl.multiple_of(g * WORDS, WORDS)
            words = [
                bit_refs[s][pl.ds(base, WORDS), pl.ds(part * LANES, LANES)] for _, part in units
            ]
            for j in range(0, WORDS, group):
                ids = [patch_ref[s, base + j + i] for i in range(group)]
                held = [out_ref[p] for p in ids]
                for i in range(group):
                    block = tile_refs[s][base + j + i].astype(jnp.float32)
                    for n, (high_rows, _) in enumerate(units):
                        rows = slice(n * ROWS, (n + 1) * ROWS)
                        samples = block[rows]
                        word = jnp.broadcast_to(words[n][j + i : j + i + 1], (ROWS, LANES))
                        one = lax.bitwise_and(word, first_masks[n]) != 0
                        two = one & (lax.bitwise_and(word, second_masks[n]) != 0)
                        counts = jnp.where(two, 1.0 + RADIX, jnp.where(one, 1.0, 0.0))
                        square = samples * samples
                        old = held[i][:, rows]
                        out_ref[ids[i], 0, rows] = old[0] + counts
                        out_ref[ids[i], 1, rows] = old[1] + jnp.where(one, samples, 0.0)
                        out_ref[ids[i], 2, rows] = old[2] + jnp.where(one, square, 0.0)
                        out_ref[ids[i], 3, rows] = old[3] + jnp.where(two, samples, 0.0)
                        out_ref[ids[i], 4, rows] = old[4] + jnp.where(two, square, 0.0)
            return 0

        lax.fori_loop(0, entries // WORDS, step, 0)


def sums_part(tiles, bits, patch_ids, patches, units):
    sources, entries, height = len(tiles), tiles[0].shape[0], ROWS * len(units)
    return pl.pallas_call(
        functools.partial(sums_kernel, units, sources),
        out_shape=jax.ShapeDtypeStruct((patches, SUMS, height, LANES), jnp.float32),
        in_specs=[pl.BlockSpec(memory_space=pltpu.SMEM)]
        + [pl.BlockSpec(memory_space=pltpu.VMEM)] * (2 * sources),
        out_specs=pl.BlockSpec(memory_space=pltpu.VMEM),
        cost_estimate=pl.CostEstimate(
            flops=50 * sources * entries * height * LANES,
            bytes_accessed=4 * patches * SUMS * height * LANES,
            transcendentals=0,
        ),
        name="sums_part",
    )(patch_ids, *tiles, *bits)


def chain(sums):
    chips, here, own = lax.axis_size("chip"), lax.axis_index("chip"), PATCH_DEV * CORES

    def local(offset):
        return lax.dynamic_slice_in_dim(sums, lax.rem(here + offset + chips, chips) * own, own, 0)

    def send(value, sign):
        return lax.ppermute(value, "chip", [(i, (i + sign) % chips) for i in range(chips)])

    up = send(local(chips // 2), 1)

    def step(i, came):
        reach = chips // 2 - i
        return send(local(reach) + came[0], 1), send(local(-reach) + came[1], -1)

    up, down = lax.fori_loop(1, chips // 2, step, (up, jnp.zeros_like(up)))
    return local(0) + up + down


def finish(sums):
    packed, sum_first, square_first, sum_both, square_both = (sums[:, i] for i in range(SUMS))
    count_both = jnp.floor(packed * (1.0 / RADIX))
    count_first = packed - count_both * RADIX
    first_mean = sum_first / jnp.maximum(count_first, 1.0)
    first_var = (square_first - sum_first * first_mean) / jnp.maximum(count_first - 1.0, 1.0)
    some = jnp.maximum(count_both, 1.0)
    shift_sum = sum_both - count_both * first_mean
    final_mean = first_mean + shift_sum / some
    final_var = (square_both - sum_both * (sum_both / some)) / jnp.maximum(count_both - 1.0, 1.0)
    return jnp.stack([first_mean, final_mean, first_var, final_var])


def per_device(visit_tiles, warp_matrix, flux_scale, patch_lists, clip_bits):
    visits, blocks, _, columns = visit_tiles.shape
    entries = visits * blocks
    chips, depth = lax.axis_size("chip"), lax.axis_size("depth")
    patches = PATCH_DEV * CORES * chips
    half = columns // CORES
    here, core = lax.axis_index("depth"), lax.axis_index("core")
    where = jnp.stack([here, core]).astype(jnp.int32)

    def place(d, c):
        return c * depth + d

    def send(value, k, h):
        if k == 0 and h == 0:
            return value
        pairs = [
            (place(d, c), place((d + k) % depth, c ^ h)) for c in range(CORES) for d in range(depth)
        ]
        return lax.ppermute(value, ("core", "depth"), pairs)

    words = clip_bits.reshape(entries, depth, CORES, half).transpose(1, 2, 0, 3)
    names = jnp.zeros((8, half), jnp.int32).at[0, :entries].set(patch_lists.reshape(entries))
    bits = []
    for k in range(depth):
        for h in range(CORES):
            message = words[lax.rem(here + k, depth), core if h == 0 else 1 - core]
            bits.append(jnp.concatenate([message, names]))
    where, bits = lax.optimization_barrier((where, bits))
    bits = [send(bits[k * CORES + h], k, h) for k in range(depth) for h in range(CORES)]
    patch_ids = jnp.stack([b[entries, :entries] for b in bits])

    pieces = []
    for chunks in (CHUNKS[:1], CHUNKS[1:]):
        pieces += warp_some(visit_tiles, warp_matrix, flux_scale, where, depth, chunks)
    sources = depth * CORES
    tiles = []
    for n in range(len(CHUNKS)):
        mine = pieces[n * sources : (n + 1) * sources]
        tiles.append([send(mine[k * CORES + h], k, h) for k in range(depth) for h in range(CORES)])
    totals = []
    for n, units in enumerate(CHUNKS):
        sums = sums_part(tiles[n], bits, patch_ids, patches, units)
        if n + 1 < len(CHUNKS):
            rows = lax.optimization_barrier(sums.reshape(-1, LANES))
            rows = lax.psum_scatter(rows, "chip", scatter_dimension=0, tiled=True)
            rows = lax.optimization_barrier(rows)
            totals.append(rows.reshape(-1, *sums.shape[1:]))
        else:
            totals.append(chain(sums))
    squares = {}
    for total, units in zip(totals, CHUNKS):
        results = finish(total)
        for n, unit in enumerate(units):
            squares[unit] = results[:, :, n * ROWS : (n + 1) * ROWS]
    results = jnp.concatenate(
        [
            jnp.concatenate([squares[r, q] for q in range(half // LANES)], axis=-1)
            for r in range(WORD_ROWS // ROWS)
        ],
        axis=-2,
    ).reshape(4, CORES, PATCH_DEV, WORD_ROWS, half)
    own, other = results[:, core], results[:, 1 - core]
    other = lax.ppermute(other, "core", [(c, c ^ 1) for c in range(CORES)])
    low, high = jnp.where(core == 0, own, other), jnp.where(core == 0, other, own)
    joined = jnp.concatenate([low, high], axis=-1)
    return joined[:2], joined[2:]


def solution(mesh):
    tracts, sky, depth = mesh.devices.shape
    fine = Mesh(
        mesh.devices.reshape(tracts, sky // CORES, CORES, depth),
        ("tracts", "chip", "core", "depth"),
    )
    every = ("tracts", "chip", "core", "depth")
    placed = (
        P(every, None, None, None),
        P(every, None, None),
        P(every),
        P(every, None),
        P(every, None, None, None),
    )
    out = P(None, ("tracts", "chip", "core"), "depth", None)

    return jax.shard_map(
        per_device, mesh=fine, in_specs=placed, out_specs=(out, out), check_vma=False
    )
```

```python
import functools

import jax
import jax.numpy as jnp
from jax import lax
from jax.experimental import pallas as pl
from jax.experimental.pallas import tpu as pltpu
from jax.sharding import Mesh
from jax.sharding import PartitionSpec as P

PATCH_DEV = 4
CORES = 2
WORD_ROWS = 16
LANES = 128
ROWS = 8
WORDS = 8
SUMS = 5
RADIX = 4096
CHUNKS = (((0, 0),), ((1, 0), (0, 1)), ((1, 1),))


def warp_kernel(depth, chunks, where_ref, scale_ref, tiles_ref, matrix_ref, *out_refs):
    here, core = where_ref[0], where_ref[1]
    factor = scale_ref[pl.program_id(0)]
    blocks, columns = tiles_ref.shape[1], tiles_ref.shape[3]
    half = columns // CORES
    width = LANES * (1 + max(part for units in chunks for _, part in units))
    low = pl.multiple_of(core * half, half)
    high = pl.multiple_of((1 - core) * half, half)
    matrix = jnp.concatenate(
        [matrix_ref[0, :, pl.ds(low, width)], matrix_ref[0, :, pl.ds(high, width)]], axis=1
    )
    for k in range(depth):
        row = pl.multiple_of(lax.rem(here + k, depth) * WORD_ROWS, WORD_ROWS)
        rows = tiles_ref[0, :, pl.ds(row, WORD_ROWS), :].reshape(blocks * WORD_ROWS, columns)
        product = jnp.dot(rows, matrix, preferred_element_type=jnp.float32) * factor
        product = product.reshape(blocks, WORD_ROWS, CORES * width)
        for n, units in enumerate(chunks):
            for h in range(CORES):
                out = out_refs[(n * depth + k) * CORES + h]
                pieces = []
                for high_rows, part in units:
                    start = h * width + part * LANES
                    pieces.append(
                        product[:, high_rows * ROWS : (high_rows + 1) * ROWS, start : start + LANES]
                    )
                piece = pieces[0] if len(pieces) == 1 else jnp.concatenate(pieces, axis=1)
                out[...] = piece.astype(jnp.bfloat16)


def warp_some(visit_tiles, warp_matrix, flux_scale, where, depth, chunks):
    visits, blocks, rows, columns = visit_tiles.shape
    heights = [ROWS * len(units) for units in chunks for _ in range(depth * CORES)]
    return pl.pallas_call(
        functools.partial(warp_kernel, depth, chunks),
        out_shape=[
            jax.ShapeDtypeStruct((visits * blocks, height, LANES), jnp.bfloat16)
            for height in heights
        ],
        grid=(visits,),
        in_specs=[
            pl.BlockSpec(memory_space=pltpu.SMEM),
            pl.BlockSpec(memory_space=pltpu.SMEM),
            pl.BlockSpec((1, blocks, rows, columns), lambda v: (v, 0, 0, 0)),
            pl.BlockSpec((1, columns, columns), lambda v: (v, 0, 0)),
        ],
        out_specs=[pl.BlockSpec((blocks, height, LANES), lambda v: (v, 0, 0)) for height in heights],
        cost_estimate=pl.CostEstimate(
            flops=2 * visits * blocks * rows * columns * columns,
            bytes_accessed=4 * visits * blocks * rows * columns,
            transcendentals=0,
        ),
        name="warp_some",
    )(where, flux_scale, visit_tiles, warp_matrix)


def sums_kernel(units, sources, patch_ref, *refs):
    tile_refs, bit_refs, out_ref = refs[:sources], refs[sources : 2 * sources], refs[-1]
    patches = out_ref.shape[0]
    entries = tile_refs[0].shape[0]
    group = 4
    positions = lax.broadcasted_iota(jnp.int32, (ROWS, LANES), 0)
    first_masks, second_masks = [], []
    for high_rows, _ in units:
        first_masks.append(lax.shift_left(jnp.ones_like(positions), positions + high_rows * ROWS))
        second_masks.append(lax.shift_left(first_masks[-1], jnp.full_like(positions, WORD_ROWS)))

    def clear(p, _):
        out_ref[p] = jnp.zeros(out_ref.shape[1:], jnp.float32)
        return 0

    lax.fori_loop(0, patches, clear, 0)
    for s in range(sources):

        def step(g, _, s=s):
            base = pl.multiple_of(g * WORDS, WORDS)
            words = [
                bit_refs[s][pl.ds(base, WORDS), pl.ds(part * LANES, LANES)] for _, part in units
            ]
            for j in range(0, WORDS, group):
                ids = [patch_ref[s, base + j + i] for i in range(group)]
                held = [out_ref[p] for p in ids]
                for i in range(group):
                    block = tile_refs[s][base + j + i].astype(jnp.float32)
                    for n, (high_rows, _) in enumerate(units):
                        rows = slice(n * ROWS, (n + 1) * ROWS)
                        samples = block[rows]
                        word = jnp.broadcast_to(words[n][j + i : j + i + 1], (ROWS, LANES))
                        one = lax.bitwise_and(word, first_masks[n]) != 0
                        two = one & (lax.bitwise_and(word, second_masks[n]) != 0)
                        counts = jnp.where(two, 1.0 + RADIX, jnp.where(one, 1.0, 0.0))
                        square = samples * samples
                        old = held[i][:, rows]
                        out_ref[ids[i], 0, rows] = old[0] + counts
                        out_ref[ids[i], 1, rows] = old[1] + jnp.where(one, samples, 0.0)
                        out_ref[ids[i], 2, rows] = old[2] + jnp.where(one, square, 0.0)
                        out_ref[ids[i], 3, rows] = old[3] + jnp.where(two, samples, 0.0)
                        out_ref[ids[i], 4, rows] = old[4] + jnp.where(two, square, 0.0)
            return 0

        lax.fori_loop(0, entries // WORDS, step, 0)


def sums_part(tiles, bits, patch_ids, patches, units):
    sources, entries, height = len(tiles), tiles[0].shape[0], ROWS * len(units)
    return pl.pallas_call(
        functools.partial(sums_kernel, units, sources),
        out_shape=jax.ShapeDtypeStruct((patches, SUMS, height, LANES), jnp.float32),
        in_specs=[pl.BlockSpec(memory_space=pltpu.SMEM)]
        + [pl.BlockSpec(memory_space=pltpu.VMEM)] * (2 * sources),
        out_specs=pl.BlockSpec(memory_space=pltpu.VMEM),
        cost_estimate=pl.CostEstimate(
            flops=50 * sources * entries * height * LANES,
            bytes_accessed=4 * patches * SUMS * height * LANES,
            transcendentals=0,
        ),
        name="sums_part",
    )(patch_ids, *tiles, *bits)


def chain(sums):
    chips, here, own = lax.axis_size("chip"), lax.axis_index("chip"), PATCH_DEV * CORES

    def local(offset):
        return lax.dynamic_slice_in_dim(sums, lax.rem(here + offset + chips, chips) * own, own, 0)

    def send(value, sign):
        return lax.ppermute(value, "chip", [(i, (i + sign) % chips) for i in range(chips)])

    up = send(local(chips // 2), 1)

    def step(i, came):
        reach = chips // 2 - i
        return send(local(reach) + came[0], 1), send(local(-reach) + came[1], -1)

    up, down = lax.fori_loop(1, chips // 2, step, (up, jnp.zeros_like(up)))
    return local(0) + up + down


def finish(sums):
    packed, sum_first, square_first, sum_both, square_both = (sums[:, i] for i in range(SUMS))
    count_both = jnp.floor(packed * (1.0 / RADIX))
    count_first = packed - count_both * RADIX
    first_mean = sum_first / jnp.maximum(count_first, 1.0)
    first_var = (square_first - sum_first * first_mean) / jnp.maximum(count_first - 1.0, 1.0)
    some = jnp.maximum(count_both, 1.0)
    shift_sum = sum_both - count_both * first_mean
    final_mean = first_mean + shift_sum / some
    final_var = (square_both - sum_both * (sum_both / some)) / jnp.maximum(count_both - 1.0, 1.0)
    return jnp.stack([first_mean, final_mean, first_var, final_var])


def per_device(visit_tiles, warp_matrix, flux_scale, patch_lists, clip_bits):
    visits, blocks, _, columns = visit_tiles.shape
    entries = visits * blocks
    chips, depth = lax.axis_size("chip"), lax.axis_size("depth")
    patches = PATCH_DEV * CORES * chips
    half = columns // CORES
    here, core = lax.axis_index("depth"), lax.axis_index("core")
    where = jnp.stack([here, core]).astype(jnp.int32)

    def place(d, c):
        return c * depth + d

    def send(value, k, h):
        if k == 0 and h == 0:
            return value
        pairs = [
            (place(d, c), place((d + k) % depth, c ^ h)) for c in range(CORES) for d in range(depth)
        ]
        return lax.ppermute(value, ("core", "depth"), pairs)

    sources = depth * CORES
    order = [(k, h) for k in range(depth) for h in range(CORES)]

    def warped(chunks):
        return warp_some(visit_tiles, warp_matrix, flux_scale, where, depth, chunks)

    def exchanged(pieces):
        return [send(piece, k, h) for piece, (k, h) in zip(pieces, order)]

    pieces = warped(CHUNKS[:1])
    pieces, clip_bits = lax.optimization_barrier((pieces, clip_bits))
    tiles = []
    tiles.append(exchanged(pieces))
    words = clip_bits.reshape(entries, depth, CORES, half).transpose(1, 2, 0, 3)
    names = jnp.zeros((8, half), jnp.int32).at[0, :entries].set(patch_lists.reshape(entries))
    bits = []
    for k, h in order:
        message = words[lax.rem(here + k, depth), core if h == 0 else 1 - core]
        bits.append(jnp.concatenate([message, names]))
    bits = exchanged(bits)
    pieces = warped(CHUNKS[1:])
    for n in range(1, len(CHUNKS)):
        tiles.append(exchanged(pieces[(n - 1) * sources : n * sources]))
    patch_ids = jnp.stack([b[entries, :entries] for b in bits])
    totals = []
    for n, units in enumerate(CHUNKS):
        sums = sums_part(tiles[n], bits, patch_ids, patches, units)
        if n + 1 < len(CHUNKS):
            rows = lax.optimization_barrier(sums.reshape(-1, LANES))
            rows = lax.psum_scatter(rows, "chip", scatter_dimension=0, tiled=True)
            rows = lax.optimization_barrier(rows)
            totals.append(rows.reshape(-1, *sums.shape[1:]))
        else:
            totals.append(chain(sums))
    squares = {}
    for total, units in zip(totals, CHUNKS):
        results = finish(total)
        for n, unit in enumerate(units):
            squares[unit] = results[:, :, n * ROWS : (n + 1) * ROWS]
    results = jnp.concatenate(
        [
            jnp.concatenate([squares[r, q] for q in range(half // LANES)], axis=-1)
            for r in range(WORD_ROWS // ROWS)
        ],
        axis=-2,
    ).reshape(4, CORES, PATCH_DEV, WORD_ROWS, half)
    own, other = results[:, core], results[:, 1 - core]
    other = lax.ppermute(other, "core", [(c, c ^ 1) for c in range(CORES)])
    low, high = jnp.where(core == 0, own, other), jnp.where(core == 0, other, own)
    joined = jnp.concatenate([low, high], axis=-1)
    return joined[:2], joined[2:]


def solution(mesh):
    tracts, sky, depth = mesh.devices.shape
    fine = Mesh(
        mesh.devices.reshape(tracts, sky // CORES, CORES, depth),
        ("tracts", "chip", "core", "depth"),
    )
    every = ("tracts", "chip", "core", "depth")
    placed = (
        P(every, None, None, None),
        P(every, None, None),
        P(every),
        P(every, None),
        P(every, None, None, None),
    )
    out = P(None, ("tracts", "chip", "core"), "depth", None)

    return jax.shard_map(
        per_device, mesh=fine, in_specs=placed, out_specs=(out, out), check_vma=False
    )
```
